8 devices in a mesh: fsdp: 8 (over z, y, x, core).
Axes of the slice: x: 2, y: 2, z: 1, core: 2. Of those that a mesh axis runs over, the one named last changes fastest.
Arguments:
- token_ids: int32 [64, 1024], P('fsdp')
- embed_table: bfloat16 [32000, 2048], P('fsdp')
- norm_gain: bfloat16 [2048], P('fsdp')
- w_query: bfloat16 [2048, 32, 64], P('fsdp')
- w_key: bfloat16 [2048, 4, 64], P('fsdp')
- w_value: bfloat16 [2048, 4, 64], P('fsdp')
- w_out: bfloat16 [2048, 2048], P('fsdp')
- grad_out: bfloat16 [64, 1024, 2048], P('fsdp')
Outputs:
- output 1: bfloat16 [64, 1024, 2048], P('fsdp')
- output 2: float32 [32000, 2048], P('fsdp')
- output 3: float32 [2048], P('fsdp')
- output 4: float32 [2048, 32, 64], P('fsdp')
- output 5: float32 [2048, 4, 64], P('fsdp')
- output 6: float32 [2048, 4, 64], P('fsdp')
- output 7: float32 [2048, 2048], P('fsdp')
All inputs are finite; a program needn't handle non-finite values.
Results may differ from the reference program's by a relative error of at most 0.00862023.
Values are sent between devices in bfloat16 or wider.
A program may use at most 1 GiB of HBM per device.

```python
import jax
import jax.numpy as jnp
from jax import lax

VOCAB_SIZE = 32000
D_MODEL = 2048
HEADS = 32
KV_HEADS = 4
HEAD_DIM = 64
GROUP_SIZE = 8
BATCH = 64
SEQ_LEN = 1024
CHUNK = 256
ROPE_THETA = 500000.0
NORM_EPS = 1e-5


def setup_inputs(seed: int = 0) -> dict:
    key_list = jax.random.split(jax.random.key(seed), 9)
    first = jax.random.randint(key_list[0], (BATCH, SEQ_LEN), 0, VOCAB_SIZE, dtype=jnp.int32)
    second = jax.random.randint(key_list[1], (BATCH, SEQ_LEN), 0, VOCAB_SIZE, dtype=jnp.int32)
    token_ids = jnp.minimum(first, second).at[0, 0].set(VOCAB_SIZE - 1)
    embed_table = (0.25 * jax.random.normal(key_list[2], (VOCAB_SIZE, D_MODEL), jnp.float32)).astype(jnp.bfloat16)
    norm_gain = (1.0 + 0.3 * jax.random.normal(key_list[3], (D_MODEL,), jnp.float32)).astype(jnp.bfloat16)
    in_scale = D_MODEL ** -0.5
    out_scale = (HEADS * HEAD_DIM) ** -0.5
    w_query = (in_scale * jax.random.normal(key_list[4], (D_MODEL, HEADS, HEAD_DIM), jnp.float32)).astype(jnp.bfloat16)
    w_key = (in_scale * jax.random.normal(key_list[5], (D_MODEL, KV_HEADS, HEAD_DIM), jnp.float32)).astype(jnp.bfloat16)
    w_value = (in_scale * jax.random.normal(key_list[6], (D_MODEL, KV_HEADS, HEAD_DIM), jnp.float32)).astype(jnp.bfloat16)
    w_out = (out_scale * jax.random.normal(key_list[7], (HEADS * HEAD_DIM, D_MODEL), jnp.float32)).astype(jnp.bfloat16)
    grad_out = jax.random.normal(key_list[8], (BATCH, SEQ_LEN, D_MODEL), jnp.float32).astype(jnp.bfloat16)
    return dict(token_ids=token_ids, embed_table=embed_table, norm_gain=norm_gain, w_query=w_query, w_key=w_key, w_value=w_value, w_out=w_out, grad_out=grad_out)


def to_bf16(values):
    return values.astype(jnp.bfloat16).astype(jnp.float32)


def rms_scale(values):
    return values * lax.rsqrt(jnp.mean(values * values, axis=-1, keepdims=True) + NORM_EPS)


def rotary(values):
    half = HEAD_DIM // 2
    frequency = ROPE_THETA ** (-2.0 * jnp.arange(half, dtype=jnp.float32) / HEAD_DIM)
    angles = jnp.arange(SEQ_LEN, dtype=jnp.float32)[:, None] * frequency[None, :]
    cosine = jnp.cos(angles)[:, None, :]
    sine = jnp.sin(angles)[:, None, :]
    first = values[..., :half]
    second = values[..., half:]
    return jnp.concatenate([first * cosine - second * sine, second * cosine + first * sine], axis=-1)


def chunk_attention(query, key_h, value):
    blocks = SEQ_LEN // CHUNK
    group = HEADS // KV_HEADS
    q_blocks = query.reshape(blocks, CHUNK, KV_HEADS, group, HEAD_DIM)
    k_blocks = key_h.reshape(blocks, CHUNK, KV_HEADS, HEAD_DIM)
    v_blocks = value.reshape(blocks, CHUNK, KV_HEADS, HEAD_DIM)
    scores = jnp.einsum('cikgd,cjkd->ckigj', q_blocks, k_blocks) * HEAD_DIM ** -0.5
    causal = jnp.arange(CHUNK)[:, None, None] >= jnp.arange(CHUNK)[None, None, :]
    attn_probs = to_bf16(jax.nn.softmax(jnp.where(causal, scores, -1e30), axis=-1))
    mixed = jnp.einsum('ckigj,cjkd->cikgd', attn_probs, v_blocks)
    return mixed.reshape(SEQ_LEN, HEADS * HEAD_DIM)


def row_forward(x_row, gain, w_query, w_key, w_value, w_out):
    normed = to_bf16(rms_scale(x_row) * gain)
    query = jnp.einsum('sd,dhe->she', normed, w_query)
    key_h = jnp.einsum('sd,dhe->she', normed, w_key)
    value = to_bf16(jnp.einsum('sd,dhe->she', normed, w_value))
    query = to_bf16(rms_scale(rotary(query)))
    key_h = to_bf16(rms_scale(rotary(key_h)))
    mixed = to_bf16(chunk_attention(query, key_h, value))
    return x_row + jnp.dot(mixed, w_out, preferred_element_type=jnp.float32)


def reference(token_ids, embed_table, norm_gain, w_query, w_key, w_value, w_out, grad_out):
    gain32 = norm_gain.astype(jnp.float32)
    query32 = w_query.astype(jnp.float32)
    key32 = w_key.astype(jnp.float32)
    value32 = w_value.astype(jnp.float32)
    wout32 = w_out.astype(jnp.float32)
    param_zero = (jnp.zeros_like(gain32), jnp.zeros_like(query32), jnp.zeros_like(key32), jnp.zeros_like(value32), jnp.zeros_like(wout32))
    table_zero = jnp.zeros((VOCAB_SIZE, D_MODEL), jnp.float32)

    def step(carry, row_inputs):
        table_acc, param_acc = carry
        row_ids, row_cot = row_inputs
        x_row = jnp.take(embed_table, row_ids, axis=0).astype(jnp.float32)
        hidden_row, pullback = jax.vjp(row_forward, x_row, gain32, query32, key32, value32, wout32)
        cotangents = pullback(row_cot.astype(jnp.float32))
        table_acc = table_acc.at[row_ids].add(cotangents[0])
        param_acc = tuple(acc + grad for acc, grad in zip(param_acc, cotangents[1:]))
        return (table_acc, param_acc), hidden_row.astype(jnp.bfloat16)

    (table_acc, param_acc), hidden = lax.scan(step, (table_zero, param_zero), (token_ids, grad_out))
    return (hidden, table_acc / GROUP_SIZE, param_acc[0] / GROUP_SIZE, param_acc[1] / GROUP_SIZE, param_acc[2] / GROUP_SIZE, param_acc[3] / GROUP_SIZE, param_acc[4] / GROUP_SIZE)
```

```python
import functools

import jax
import jax.numpy as jnp
from jax import lax
from jax.experimental import pallas as pl
from jax.experimental.pallas import tpu as pltpu
from jax.sharding import PartitionSpec as P


ROPE_THETA = 500000.0
NORM_EPS = 1e-5
WINDOWS = 4
LANES = 128
ROWS = 256
PARTS = 4
RUN = 128

NT = (((1,), (1,)), ((), ()))
F32 = jnp.float32
BF16 = jnp.bfloat16


def split_kernel(table_ref, out_ref, wide):
    rows, width = table_ref.shape
    slabs = width // LANES
    for j in range(slabs):
        wide[pl.ds(j, rows, stride=slabs), :] = table_ref[:, j * LANES : (j + 1) * LANES].astype(F32)
    out_ref[...] = wide[...].reshape(rows, slabs, LANES).astype(BF16)


def split_rows(table, block=200):
    rows, width = table.shape
    slabs = width // LANES
    return pl.pallas_call(
        split_kernel,
        grid=(rows // block,),
        out_shape=jax.ShapeDtypeStruct((rows, slabs, LANES), BF16),
        in_specs=[pl.BlockSpec((block, width), lambda i: (i, 0))],
        out_specs=pl.BlockSpec((block, slabs, LANES), lambda i: (i, 0, 0)),
        scratch_shapes=[pltpu.VMEM((block * slabs, LANES), F32)],
        cost_estimate=pl.CostEstimate(flops=rows * width, bytes_accessed=4 * rows * width, transcendentals=0),
        name='split_rows',
    )(table)


def join_kernel(scale, part_ref, *refs):
    out_ref, wide = refs[-2:]
    rows, width = out_ref.shape
    slabs = width // LANES
    wide[...] = part_ref[...].astype(F32).reshape(rows * slabs, LANES) * scale
    for j in range(slabs):
        out_ref[:, j * LANES : (j + 1) * LANES] = wide[pl.ds(j, rows, stride=slabs), :]


def join_rows(part, whole, index, count, scale, block=200):
    rows, slabs, _ = part.shape
    width = slabs * LANES
    steps = rows // block
    in_specs = [pl.BlockSpec((block, slabs, LANES), lambda i: (i, 0, 0))]
    operands = [part]
    aliases = {}
    if whole is not None:
        in_specs.append(pl.BlockSpec(memory_space=pl.ANY))
        operands.append(whole)
        aliases = {1: 0}
    return pl.pallas_call(
        functools.partial(join_kernel, scale),
        grid=(steps,),
        out_shape=jax.ShapeDtypeStruct((rows * count, width), F32),
        in_specs=in_specs,
        out_specs=pl.BlockSpec((block, width), lambda i: (index * steps + i, 0)),
        scratch_shapes=[pltpu.VMEM((block * slabs, LANES), F32)],
        input_output_aliases=aliases,
        cost_estimate=pl.CostEstimate(flops=rows * width, bytes_accessed=6 * rows * width, transcendentals=0),
        name='join_rows',
    )(*operands)


def embed_kernel(ids_ref, table_ref, gain_ref, weight_ref, x_ref, normed_ref, raw_ref, fetched, wide, sems):
    step, steps = pl.program_id(0), pl.num_programs(0)
    rows, width = x_ref.shape
    slabs = width // LANES

    def fetch(block, slot):
        def one(t, carry):
            pltpu.make_async_copy(table_ref.at[ids_ref[block * rows + t]], fetched.at[slot, t], sems.at[slot]).start()
            return carry

        lax.fori_loop(0, rows, one, 0, unroll=8)

    @pl.when(step == 0)
    def _():
        fetch(0, 0)

    @pl.when(step + 1 < steps)
    def _():
        fetch(step + 1, lax.rem(step + 1, 2))

    slot = lax.rem(step, 2)
    pltpu.make_async_copy(table_ref.at[pl.ds(0, rows)], fetched.at[slot], sems.at[slot]).wait()
    wide[...] = fetched[slot].astype(F32).reshape(rows * slabs, LANES)
    square = jnp.zeros((rows, LANES), F32)
    for j in range(slabs):
        x_part = wide[pl.ds(j, rows, stride=slabs), :]
        square += x_part * x_part
        x_ref[:, j * LANES : (j + 1) * LANES] = x_part.astype(BF16)
    scale = lax.rsqrt(jnp.sum(square, axis=1, keepdims=True) * (1.0 / width) + NORM_EPS)
    for j in range(slabs):
        cols = slice(j * LANES, (j + 1) * LANES)
        normed_ref[:, cols] = (x_ref[:, cols].astype(F32) * scale * gain_ref[:, cols]).astype(BF16)
    raw_ref[0] = lax.dot_general(weight_ref[...], normed_ref[...], NT, preferred_element_type=F32)


def embed_project(ids, table, gain, weight_t):
    tokens = ids.shape[0]
    slabs = table.shape[1]
    features, width = weight_t.shape
    steps = tokens // ROWS
    return pl.pallas_call(
        embed_kernel,
        grid_spec=pltpu.PrefetchScalarGridSpec(
            num_scalar_prefetch=1,
            grid=(steps,),
            in_specs=[
                pl.BlockSpec(memory_space=pl.ANY),
                pl.BlockSpec((1, width), lambda i, ids: (0, 0)),
                pl.BlockSpec((features, width), lambda i, ids: (0, 0)),
            ],
            out_specs=[
                pl.BlockSpec((ROWS, width), lambda i, ids: (i, 0)),
                pl.BlockSpec((ROWS, width), lambda i, ids: (i, 0)),
                pl.BlockSpec((1, features, ROWS), lambda i, ids: (i, 0, 0)),
            ],
            scratch_shapes=[
                pltpu.VMEM((2, ROWS, slabs, LANES), BF16),
                pltpu.VMEM((ROWS * slabs, LANES), F32),
                pltpu.SemaphoreType.DMA((2,)),
            ],
        ),
        out_shape=[
            jax.ShapeDtypeStruct((tokens, width), BF16),
            jax.ShapeDtypeStruct((tokens, width), BF16),
            jax.ShapeDtypeStruct((steps, features, ROWS), F32),
        ],
        cost_estimate=pl.CostEstimate(flops=2 * tokens * width * features, bytes_accessed=tokens * (6 * width + 4 * features), transcendentals=tokens),
        name='embed_project',
    )(ids, table, gain, weight_t)


def rotate(values, cosine, sine):
    half = values.shape[0] // 2
    first, second = values[:half], values[half:]
    return jnp.concatenate([first * cosine - second * sine, second * cosine + first * sine], axis=0)


def rotate_back(values, cosine, sine):
    half = values.shape[0] // 2
    first, second = values[:half], values[half:]
    return jnp.concatenate([first * cosine + second * sine, second * cosine - first * sine], axis=0)


def head_norm(values):
    scale = lax.rsqrt(jnp.mean(values * values, axis=0, keepdims=True) + NORM_EPS)
    return values * scale, scale


def head_norm_back(grads, unit, scale):
    return scale * (grads - unit * jnp.mean(unit * grads, axis=0, keepdims=True))


def attention_kernel(group, dim, raw_ref, dmix_ref, cos_ref, sin_ref, mix_ref, draw_ref):
    tokens = raw_ref.shape[2]
    half = tokens // 2
    cosine, sine = cos_ref[...], sin_ref[...]
    k_unit, k_scale = head_norm(rotate(raw_ref[0, group * dim : (group + 1) * dim, :], cosine, sine))
    key_t = k_unit.astype(BF16)
    key_f = key_t.astype(F32) * dim**-0.5
    key_small_t = key_f.astype(BF16)
    key_small = key_f.T.astype(BF16)
    value_f = raw_ref[0, (group + 1) * dim : (group + 2) * dim, :].astype(BF16)
    value_t = value_f
    value = value_f.astype(F32).T.astype(BF16)
    keys_at = lax.broadcasted_iota(jnp.int32, (half, half), 0)
    queries_at = lax.broadcasted_iota(jnp.int32, (half, half), 1)
    causal = queries_at >= keys_at
    empty = jnp.zeros((half, half), BF16)
    d_key = jnp.zeros((dim, tokens), F32)
    d_value = jnp.zeros((dim, tokens), F32)
    for head in range(group):
        rows = slice(head * dim, (head + 1) * dim)
        q_unit, q_scale = head_norm(rotate(raw_ref[0, rows, :], cosine, sine))
        query_t = q_unit.astype(BF16)
        d_out = dmix_ref[rows, :]
        scores = jnp.dot(key_small, query_t, preferred_element_type=F32)
        d_probs = jnp.dot(value, d_out, preferred_element_type=F32)
        early = jnp.where(causal, jnp.exp(scores[:half, :half]), 0.0)
        cross = jnp.exp(scores[:half, half:])
        late = jnp.where(causal, jnp.exp(scores[half:, half:]), 0.0)
        early_inv = 1.0 / jnp.sum(early, axis=0, keepdims=True)
        late_inv = 1.0 / (jnp.sum(cross, axis=0, keepdims=True) + jnp.sum(late, axis=0, keepdims=True))
        early, cross, late = early * early_inv, cross * late_inv, late * late_inv
        probs = jnp.concatenate(
            [
                jnp.concatenate([early.astype(BF16), cross.astype(BF16)], axis=1),
                jnp.concatenate([empty, late.astype(BF16)], axis=1),
            ],
            axis=0,
        )
        mix_ref[rows, :] = jnp.dot(value_t, probs, preferred_element_type=F32).astype(BF16)
        d_early, d_cross, d_late = d_probs[:half, :half], d_probs[:half, half:], d_probs[half:, half:]
        early_dot = jnp.sum(early * d_early, axis=0, keepdims=True)
        late_dot = jnp.sum(cross * d_cross, axis=0, keepdims=True) + jnp.sum(late * d_late, axis=0, keepdims=True)
        d_scores = jnp.concatenate(
            [
                jnp.concatenate([(early * (d_early - early_dot)).astype(BF16), (cross * (d_cross - late_dot)).astype(BF16)], axis=1),
                jnp.concatenate([empty, (late * (d_late - late_dot)).astype(BF16)], axis=1),
            ],
            axis=0,
        )
        d_query = jnp.dot(key_small_t, d_scores, preferred_element_type=F32)
        d_key += lax.dot_general(query_t, d_scores, NT, preferred_element_type=F32)
        d_value += lax.dot_general(d_out, probs, NT, preferred_element_type=F32)
        draw_ref[rows, :] = rotate_back(head_norm_back(d_query, q_unit, q_scale), cosine, sine).astype(BF16)
    d_key = rotate_back(head_norm_back(d_key * dim**-0.5, k_unit, k_scale), cosine, sine)
    draw_ref[group * dim : (group + 1) * dim, :] = d_key.astype(BF16)
    draw_ref[(group + 1) * dim :, :] = d_value.astype(BF16)


def attention(raw, d_mixed_t, cosine, sine, kv_heads, group, dim):
    steps, features, tokens = raw.shape
    block = features // kv_heads
    width = group * dim
    pairs = steps * kv_heads * group * tokens * tokens
    return pl.pallas_call(
        functools.partial(attention_kernel, group, dim),
        grid=(steps, kv_heads),
        in_specs=[
            pl.BlockSpec((1, block, tokens), lambda w, k: (w, k, 0)),
            pl.BlockSpec((width, tokens), lambda w, k: (k, w)),
            pl.BlockSpec((dim // 2, tokens), lambda w, k: (0, w % WINDOWS)),
            pl.BlockSpec((dim // 2, tokens), lambda w, k: (0, w % WINDOWS)),
        ],
        out_specs=[
            pl.BlockSpec((width, tokens), lambda w, k: (k, w)),
            pl.BlockSpec((block, tokens), lambda w, k: (k, w)),
        ],
        out_shape=[
            jax.ShapeDtypeStruct((width * kv_heads, steps * tokens), BF16),
            jax.ShapeDtypeStruct((features, steps * tokens), BF16),
        ],
        cost_estimate=pl.CostEstimate(flops=12 * pairs * dim, bytes_accessed=8 * raw.size, transcendentals=pairs),
        name='attention',
    )(raw, d_mixed_t, cosine, sine)


def input_grad_kernel(place_ref, draw_ref, weight_ref, x_ref, dh_ref, gain_ref, sorted_ref, dgain_ref, d_normed, wide, sems):
    step, steps = pl.program_id(0), pl.num_programs(0)
    rows, width = x_ref.shape
    slabs = width // LANES
    slot = lax.rem(step, 2)

    def drain(which):
        pltpu.make_async_copy(wide.at[which], sorted_ref.at[pl.ds(0, rows * slabs)], sems.at[which]).wait()

    d_normed[...] = jnp.dot(draw_ref[...].T, weight_ref[...], preferred_element_type=F32)
    square = jnp.zeros((rows, LANES), F32)
    cross = jnp.zeros((rows, LANES), F32)
    for j in range(slabs):
        cols = slice(j * LANES, (j + 1) * LANES)
        x_part = x_ref[:, cols].astype(F32)
        square += x_part * x_part
        cross += x_part * d_normed[:, cols] * gain_ref[:, cols]
    scale = lax.rsqrt(jnp.sum(square, axis=1, keepdims=True) * (1.0 / width) + NORM_EPS)
    pull = jnp.sum(cross, axis=1, keepdims=True) * (1.0 / width) * scale * scale

    @pl.when(step == 0)
    def _():
        dgain_ref[...] = jnp.zeros_like(dgain_ref)

    @pl.when(step >= 2)
    def _():
        drain(slot)

    for j in range(slabs):
        cols = slice(j * LANES, (j + 1) * LANES)
        x_part = x_ref[:, cols].astype(F32)
        d_part = d_normed[:, cols]
        dx_part = dh_ref[:, cols].astype(F32) + scale * (d_part * gain_ref[:, cols] - x_part * pull)
        wide[slot, pl.ds(j, rows, stride=slabs), :] = dx_part
        terms = d_part * (x_part * scale)
        dgain_ref[:, cols] += jnp.sum(terms.reshape(rows // 8, 8, LANES), axis=0)

    def one(t, carry):
        source = wide.at[slot, pl.ds(pl.multiple_of(t * slabs, slabs), slabs)]
        start = pl.multiple_of(place_ref[step * rows + t] * slabs, slabs)
        pltpu.make_async_copy(source, sorted_ref.at[pl.ds(start, slabs)], sems.at[slot]).start()
        return carry

    lax.fori_loop(0, rows, one, 0, unroll=8)

    @pl.when(step == steps - 1)
    def _():
        drain(1 - slot)
        drain(slot)


def input_grad(place, draw_t, weight_t, x, dh, gain, spare):
    tokens, width = x.shape
    slabs = width // LANES
    features = draw_t.shape[0]
    steps = tokens // ROWS
    return pl.pallas_call(
        input_grad_kernel,
        grid_spec=pltpu.PrefetchScalarGridSpec(
            num_scalar_prefetch=1,
            grid=(steps,),
            in_specs=[
                pl.BlockSpec((features, ROWS), lambda i, place: (0, i)),
                pl.BlockSpec((features, width), lambda i, place: (0, 0)),
                pl.BlockSpec((ROWS, width), lambda i, place: (i, 0)),
                pl.BlockSpec((ROWS, width), lambda i, place: (i, 0)),
                pl.BlockSpec((1, width), lambda i, place: (0, 0)),
            ],
            out_specs=[
                pl.BlockSpec(memory_space=pl.ANY),
                pl.BlockSpec((8, width), lambda i, place: (0, 0)),
            ],
            scratch_shapes=[
                pltpu.VMEM((ROWS, width), F32),
                pltpu.VMEM((2, ROWS * slabs, LANES), F32),
                pltpu.SemaphoreType.DMA((2,)),
            ],
        ),
        out_shape=[
            jax.ShapeDtypeStruct(((tokens + spare) * slabs, LANES), F32),
            jax.ShapeDtypeStruct((8, width), F32),
        ],
        cost_estimate=pl.CostEstimate(flops=2 * tokens * width * features, bytes_accessed=tokens * (8 * width + 2 * features), transcendentals=tokens),
        name='input_grad',
    )(place, draw_t, weight_t, x, dh, gain)


def table_grad_kernel(bounds_ref, same_ref, target_ref, sorted_ref, zero_ref, out_ref, fetched, summed, in_sems, out_sems):
    del zero_ref
    slabs = out_ref.shape[1]
    first, last = bounds_ref[0], bounds_ref[1]
    steps = lax.div(last - first + (RUN - 1), RUN)

    def fetch(step, slot):
        start = pl.multiple_of((first + step * RUN) * slabs, slabs)
        return pltpu.make_async_copy(sorted_ref.at[pl.ds(start, RUN * slabs)], fetched.at[slot], in_sems.at[slot])

    def drain(count, slot):
        for bit in range(RUN.bit_length()):

            @pl.when(lax.rem(lax.div(count, 1 << bit), 2) == 1)
            def _():
                pltpu.make_async_copy(summed.at[slot, pl.ds(0, 1 << bit)], out_ref.at[pl.ds(0, 1 << bit)], out_sems.at[slot]).wait()

    @pl.when(steps > 0)
    def _():
        fetch(0, 0).start()

    def step_body(step, carry):
        total, older, newer = carry
        slot = lax.rem(step, 2)

        @pl.when(step + 1 < steps)
        def _():
            fetch(step + 1, 1 - slot).start()

        fetch(step, slot).wait()
        drain(older, slot)
        base = first + step * RUN

        def add(t, total):
            row = fetched[slot, pl.ds(pl.multiple_of(t * slabs, slabs), slabs), :]
            total = row + jnp.where(same_ref[base + t] == 1, total, 0.0)
            summed[slot, t] = total.astype(BF16)
            return total

        total = lax.fori_loop(0, RUN, add, total, unroll=8)

        def send(t, count):
            target = target_ref[base + t]
            wanted = jnp.logical_and(target >= 0, base + t < last)

            @pl.when(wanted)
            def _():
                pltpu.make_async_copy(summed.at[slot, t], out_ref.at[target], out_sems.at[slot]).start()

            return count + wanted.astype(jnp.int32)

        count = lax.fori_loop(0, RUN, send, jnp.int32(0), unroll=8)
        return total, newer, count

    zero = jnp.int32(0)
    _, older, newer = lax.fori_loop(0, steps, step_body, (jnp.zeros((slabs, LANES), F32), zero, zero))
    drain(older, lax.rem(steps, 2))
    drain(newer, lax.rem(steps + 1, 2))


def table_grad(bounds, same, target, sorted_rows, zero_part):
    rows, slabs, _ = zero_part.shape
    return pl.pallas_call(
        table_grad_kernel,
        grid_spec=pltpu.PrefetchScalarGridSpec(
            num_scalar_prefetch=3,
            grid=(),
            in_specs=[pl.BlockSpec(memory_space=pl.ANY), pl.BlockSpec(memory_space=pl.ANY)],
            out_specs=pl.BlockSpec(memory_space=pl.ANY),
            scratch_shapes=[
                pltpu.VMEM((2, RUN * slabs, LANES), F32),
                pltpu.VMEM((2, RUN, slabs, LANES), BF16),
                pltpu.SemaphoreType.DMA((2,)),
                pltpu.SemaphoreType.DMA((2,)),
            ],
        ),
        out_shape=jax.ShapeDtypeStruct((rows, slabs, LANES), BF16),
        input_output_aliases={4: 0},
        cost_estimate=pl.CostEstimate(flops=sorted_rows.size // PARTS, bytes_accessed=6 * sorted_rows.size // PARTS, transcendentals=0),
        name='table_grad',
    )(bounds, same, target, sorted_rows, zero_part)


def zero_kernel(*refs):
    *out_refs, block, sem = refs
    block[...] = jnp.zeros_like(block)
    rows = block.shape[0]
    copies = [pltpu.make_async_copy(block, ref.at[pl.ds(start, rows)], sem) for ref in out_refs for start in range(0, ref.shape[0], rows)]
    for copy in copies:
        copy.start()
    for copy in copies:
        copy.wait()


def zero_tables(count, rows, slabs, block=400):
    return pl.pallas_call(
        zero_kernel,
        out_shape=[jax.ShapeDtypeStruct((rows, slabs, LANES), BF16)] * count,
        out_specs=[pl.BlockSpec(memory_space=pl.ANY)] * count,
        scratch_shapes=[pltpu.VMEM((block, slabs, LANES), BF16), pltpu.SemaphoreType.DMA],
        cost_estimate=pl.CostEstimate(flops=count * rows * slabs * LANES, bytes_accessed=2 * count * rows * slabs * LANES, transcendentals=0),
        name='zero_tables',
    )()


def solution(mesh):
    devices = mesh.shape['fsdp']

    def device_step(token_ids, embed_table, norm_gain, w_query, w_key, w_value, w_out, grad_out):
        batch, seq_len = token_ids.shape
        table_rows, width = embed_table.shape
        heads, dim = w_query.shape[1], w_query.shape[2]
        kv_heads = w_key.shape[1]
        group = heads // kv_heads
        tokens = batch * seq_len
        slabs = width // LANES
        ids = token_ids.reshape(tokens)
        dh = grad_out.reshape(tokens, width)

        def grouped(w, count):
            return w.transpose(1, 2, 0).reshape(kv_heads, count * dim, -1)

        weight_part = jnp.concatenate([grouped(w_query, group), grouped(w_key, 1), grouped(w_value, 1)], axis=1)
        weight_part = weight_part.reshape(-1, weight_part.shape[-1])
        wout_full = lax.all_gather(w_out, 'fsdp', axis=0, tiled=True)
        weight_t = lax.all_gather(weight_part, 'fsdp', axis=1, tiled=True)
        gain = lax.all_gather(norm_gain, 'fsdp', axis=0, tiled=True).astype(F32).reshape(1, width)
        table = lax.all_gather(split_rows(embed_table), 'fsdp', axis=0, tiled=True)

        piece = table_rows // PARTS
        part_rows = piece * devices
        local = ids % table_rows
        key = (local // piece) * part_rows + (ids // table_rows) * piece + local % piece
        count = jnp.arange(tokens, dtype=jnp.int32)
        sorted_key, order = lax.sort((key, count), num_keys=1)
        _, place = lax.sort((order, count), num_keys=1)
        outside = jnp.full((1,), -1, jnp.int32)
        same = (sorted_key == jnp.concatenate([outside, sorted_key[:-1]])).astype(jnp.int32)
        ends = sorted_key != jnp.concatenate([sorted_key[1:], outside])
        target = jnp.where(ends, sorted_key % part_rows, -1)
        spare = jnp.zeros((RUN,), jnp.int32)
        same = jnp.concatenate([same, spare])
        target = jnp.concatenate([target, spare - 1])
        bounds = jnp.sum(key[None, :] < part_rows * jnp.arange(PARTS + 1, dtype=jnp.int32)[:, None], axis=1, dtype=jnp.int32)

        half = dim // 2
        frequency = ROPE_THETA ** (-2.0 * jnp.arange(half, dtype=F32) / dim)
        angles = frequency[:, None] * jnp.arange(seq_len, dtype=F32)[None, :]
        cosine, sine = jnp.cos(angles), jnp.sin(angles)

        d_mixed_t = lax.dot_general(wout_full, dh, NT, preferred_element_type=F32).astype(BF16)
        zero_parts = zero_tables(PARTS, part_rows, slabs)
        d_mixed_t, *zero_parts = lax.optimization_barrier((d_mixed_t, *zero_parts))

        x, normed, raw = embed_project(ids, table, gain, weight_t)
        mixed_t, draw_t = attention(raw, d_mixed_t, cosine, sine, kv_heads, group, dim)
        sorted_rows, dgain = input_grad(place, draw_t, weight_t, x, dh, gain, RUN)
        parts = [table_grad(bounds[k : k + 2], same, target, sorted_rows, zero_parts[k]) for k in range(PARTS)]
        shares = []
        for k in range(PARTS):
            shares.append(lax.psum_scatter(parts[k], 'fsdp', scatter_dimension=0, tiled=True))
        grad_table = None
        for k in range(PARTS):
            grad_table = join_rows(shares[k], grad_table, k, PARTS, 1.0 / devices)

        mixed_t, draw_t, *_ = lax.optimization_barrier((mixed_t, draw_t, *parts))
        grad_weight = jnp.dot(draw_t, normed, preferred_element_type=F32).astype(BF16)
        grad_weight = lax.psum_scatter(grad_weight, 'fsdp', scatter_dimension=1, tiled=True)
        grad_weight = grad_weight.astype(F32) / devices
        grad_wout = jnp.dot(mixed_t, dh, preferred_element_type=F32).astype(BF16)
        grad_wout = lax.psum_scatter(grad_wout, 'fsdp', scatter_dimension=0, tiled=True)
        grad_wout = grad_wout.astype(F32) / devices
        hidden = x.astype(F32) + lax.dot_general(mixed_t, wout_full, (((0,), (0,)), ((), ())), preferred_element_type=F32)
        hidden = hidden.astype(BF16).reshape(batch, seq_len, width)
        grad_gain = lax.psum_scatter(jnp.sum(dgain, axis=0), 'fsdp', scatter_dimension=0, tiled=True) / devices

        grad_weight = grad_weight.reshape(kv_heads, (group + 2) * dim, -1)

        def ungrouped(part, count):
            return part.reshape(kv_heads * count, dim, -1).transpose(2, 0, 1)

        grad_query = ungrouped(grad_weight[:, : group * dim], group)
        grad_key = ungrouped(grad_weight[:, group * dim : (group + 1) * dim], 1)
        grad_value = ungrouped(grad_weight[:, (group + 1) * dim :], 1)
        return hidden, grad_table, grad_gain, grad_query, grad_key, grad_value, grad_wout

    tokens = P('fsdp', None, None)
    matrix = P('fsdp', None)
    vector = P('fsdp')
    return jax.shard_map(device_step, mesh=mesh, in_specs=(matrix, matrix, vector, tokens, tokens, tokens, matrix, tokens), out_specs=(tokens, matrix, vector, tokens, tokens, tokens, matrix), check_vma=False)
```

```python
import functools

import jax
import jax.numpy as jnp
from jax import lax
from jax.experimental import pallas as pl
from jax.experimental.pallas import tpu as pltpu
from jax.sharding import PartitionSpec as P


ROPE_THETA = 500000.0
NORM_EPS = 1e-5
WINDOWS = 4
LANES = 128
ROWS = 256
HALVES = 2
PARTS = 4
RUN = 128

NT = (((1,), (1,)), ((), ()))
F32 = jnp.float32
BF16 = jnp.bfloat16


def split_kernel(table_ref, out_ref, wide):
    rows, width = table_ref.shape
    slabs = width // LANES
    for j in range(slabs):
        wide[pl.ds(j, rows, stride=slabs), :] = table_ref[:, j * LANES : (j + 1) * LANES].astype(F32)
    out_ref[...] = wide[...].reshape(rows, slabs, LANES).astype(BF16)


def split_rows(table, block=200):
    rows, width = table.shape
    slabs = width // LANES
    return pl.pallas_call(
        split_kernel,
        grid=(rows // block,),
        out_shape=jax.ShapeDtypeStruct((rows, slabs, LANES), BF16),
        in_specs=[pl.BlockSpec((block, width), lambda i: (i, 0))],
        out_specs=pl.BlockSpec((block, slabs, LANES), lambda i: (i, 0, 0)),
        scratch_shapes=[pltpu.VMEM((block * slabs, LANES), F32)],
        cost_estimate=pl.CostEstimate(flops=rows * width, bytes_accessed=4 * rows * width, transcendentals=0),
        name='split_rows',
    )(table)


def join_kernel(scale, part_ref, *refs):
    out_ref, wide = refs[-2:]
    rows, width = out_ref.shape
    slabs = width // LANES
    wide[...] = part_ref[...].astype(F32).reshape(rows * slabs, LANES) * scale
    for j in range(slabs):
        out_ref[:, j * LANES : (j + 1) * LANES] = wide[pl.ds(j, rows, stride=slabs), :]


def join_rows(part, whole, half, index, scale, block=200):
    rows, slabs, _ = part.shape
    width = slabs * LANES
    steps = rows // block
    in_specs = [pl.BlockSpec((block, slabs, LANES), lambda i: (i, 0, 0))]
    operands = [part]
    aliases = {}
    if whole is not None:
        in_specs.append(pl.BlockSpec(memory_space=pl.ANY))
        operands.append(whole)
        aliases = {1: 0}
    return pl.pallas_call(
        functools.partial(join_kernel, scale),
        grid=(steps,),
        out_shape=jax.ShapeDtypeStruct((rows * PARTS, width * HALVES), F32),
        in_specs=in_specs,
        out_specs=pl.BlockSpec((block, width), lambda i: (index * steps + i, half)),
        scratch_shapes=[pltpu.VMEM((block * slabs, LANES), F32)],
        input_output_aliases=aliases,
        cost_estimate=pl.CostEstimate(flops=rows * width, bytes_accessed=6 * rows * width, transcendentals=0),
        name='join_rows',
    )(*operands)


def embed_kernel(ids_ref, table_ref, gain_ref, weight_ref, x_ref, normed_ref, scale_ref, raw_ref, fetched, wide, sems):
    step, steps = pl.program_id(0), pl.num_programs(0)
    rows, width = x_ref.shape
    slabs = width // LANES

    def fetch(block, slot):
        def one(t, carry):
            pltpu.make_async_copy(table_ref.at[ids_ref[block * rows + t]], fetched.at[slot, t], sems.at[slot]).start()
            return carry

        lax.fori_loop(0, rows, one, 0, unroll=8)

    @pl.when(step == 0)
    def _():
        fetch(0, 0)

    @pl.when(step + 1 < steps)
    def _():
        fetch(step + 1, lax.rem(step + 1, 2))

    slot = lax.rem(step, 2)
    pltpu.make_async_copy(table_ref.at[pl.ds(0, rows)], fetched.at[slot], sems.at[slot]).wait()
    wide[...] = fetched[slot].astype(F32).reshape(rows * slabs, LANES)
    square = jnp.zeros((rows, LANES), F32)
    for j in range(slabs):
        x_part = wide[pl.ds(j, rows, stride=slabs), :]
        square += x_part * x_part
        x_ref[:, j * LANES : (j + 1) * LANES] = x_part.astype(BF16)
    scale = lax.rsqrt(jnp.sum(square, axis=1, keepdims=True) * (1.0 / width) + NORM_EPS)
    scale = jnp.broadcast_to(scale, (rows, LANES))
    scale_ref[...] = scale
    for j in range(slabs):
        cols = slice(j * LANES, (j + 1) * LANES)
        normed_ref[:, cols] = (x_ref[:, cols].astype(F32) * scale * gain_ref[:, cols]).astype(BF16)
    raw_ref[0] = lax.dot_general(weight_ref[...], normed_ref[...], NT, preferred_element_type=F32)


def embed_project(ids, table, gain, weight_t):
    tokens = ids.shape[0]
    slabs = table.shape[1]
    features, width = weight_t.shape
    steps = tokens // ROWS
    return pl.pallas_call(
        embed_kernel,
        grid_spec=pltpu.PrefetchScalarGridSpec(
            num_scalar_prefetch=1,
            grid=(steps,),
            in_specs=[
                pl.BlockSpec(memory_space=pl.ANY),
                pl.BlockSpec((1, width), lambda i, ids: (0, 0)),
                pl.BlockSpec((features, width), lambda i, ids: (0, 0)),
            ],
            out_specs=[
                pl.BlockSpec((ROWS, width), lambda i, ids: (i, 0)),
                pl.BlockSpec((ROWS, width), lambda i, ids: (i, 0)),
                pl.BlockSpec((ROWS, LANES), lambda i, ids: (i, 0)),
                pl.BlockSpec((1, features, ROWS), lambda i, ids: (i, 0, 0)),
            ],
            scratch_shapes=[
                pltpu.VMEM((2, ROWS, slabs, LANES), BF16),
                pltpu.VMEM((ROWS * slabs, LANES), F32),
                pltpu.SemaphoreType.DMA((2,)),
            ],
        ),
        out_shape=[
            jax.ShapeDtypeStruct((tokens, width), BF16),
            jax.ShapeDtypeStruct((tokens, width), BF16),
            jax.ShapeDtypeStruct((tokens, LANES), F32),
            jax.ShapeDtypeStruct((steps, features, ROWS), F32),
        ],
        cost_estimate=pl.CostEstimate(flops=2 * tokens * width * features, bytes_accessed=tokens * (6 * width + 4 * features), transcendentals=tokens),
        name='embed_project',
    )(ids, table, gain, weight_t)


def rotate(values, cosine, sine):
    half = values.shape[0] // 2
    first, second = values[:half], values[half:]
    return jnp.concatenate([first * cosine - second * sine, second * cosine + first * sine], axis=0)


def rotate_back(values, cosine, sine):
    half = values.shape[0] // 2
    first, second = values[:half], values[half:]
    return jnp.concatenate([first * cosine + second * sine, second * cosine - first * sine], axis=0)


def head_norm(values):
    scale = lax.rsqrt(jnp.mean(values * values, axis=0, keepdims=True) + NORM_EPS)
    return values * scale, scale


def head_norm_back(grads, unit, scale):
    return scale * (grads - unit * jnp.mean(unit * grads, axis=0, keepdims=True))


def softmax_and_grad(scores, d_probs, causal, empty):
    half = scores.shape[0] // 2
    early = jnp.where(causal, jnp.exp(scores[:half, :half]), 0.0)
    cross = jnp.exp(scores[:half, half:])
    late = jnp.where(causal, jnp.exp(scores[half:, half:]), 0.0)
    early_inv = 1.0 / jnp.sum(early, axis=0, keepdims=True)
    late_inv = 1.0 / jnp.sum(cross + late, axis=0, keepdims=True)
    early, cross, late = early * early_inv, cross * late_inv, late * late_inv
    probs = jnp.concatenate(
        [
            jnp.concatenate([early.astype(BF16), cross.astype(BF16)], axis=1),
            jnp.concatenate([empty, late.astype(BF16)], axis=1),
        ],
        axis=0,
    )
    d_early, d_cross, d_late = d_probs[:half, :half], d_probs[:half, half:], d_probs[half:, half:]
    early_dot = jnp.sum(early * d_early, axis=0, keepdims=True)
    late_dot = jnp.sum(cross * d_cross + late * d_late, axis=0, keepdims=True)
    d_scores = jnp.concatenate(
        [
            jnp.concatenate([(early * (d_early - early_dot)).astype(BF16), (cross * (d_cross - late_dot)).astype(BF16)], axis=1),
            jnp.concatenate([empty, (late * (d_late - late_dot)).astype(BF16)], axis=1),
        ],
        axis=0,
    )
    return probs, d_scores


def attention_kernel(kv_heads, group, dim, raw_ref, dmix_ref, cos_ref, sin_ref, mix_ref, draw_ref, pull_ref):
    tokens = raw_ref.shape[2]
    half = tokens // 2
    block = (group + 2) * dim
    cosine, sine = cos_ref[...], sin_ref[...]
    keys_at = lax.broadcasted_iota(jnp.int32, (half, half), 0)
    queries_at = lax.broadcasted_iota(jnp.int32, (half, half), 1)
    causal = queries_at >= keys_at
    empty = jnp.zeros((half, half), BF16)

    def one_kv_head(kv, pull):
        def rows(at):
            return pl.ds(pl.multiple_of(kv * block + at * dim, dim), dim)

        def mixed_rows(head):
            return pl.ds(pl.multiple_of((kv * group + head) * dim, dim), dim)

        def put(at, values):
            values = values.astype(BF16)
            draw_ref[rows(at), :] = values
            return values.astype(F32) * raw_ref[0, rows(at), :]

        k_unit, k_scale = head_norm(rotate(raw_ref[0, rows(group), :], cosine, sine))
        key_f = k_unit.astype(BF16).astype(F32) * dim**-0.5
        key_small_t = key_f.astype(BF16)
        key_small = key_f.T.astype(BF16)
        value_t = raw_ref[0, rows(group + 1), :].astype(BF16)
        value = value_t.astype(F32).T.astype(BF16)
        d_key = jnp.zeros((dim, tokens), F32)
        d_value = jnp.zeros((dim, tokens), F32)

        def begin(head):
            q_unit, q_scale = head_norm(rotate(raw_ref[0, rows(head), :], cosine, sine))
            query_t = q_unit.astype(BF16)
            d_out = dmix_ref[mixed_rows(head), :]
            scores = jnp.dot(key_small, query_t, preferred_element_type=F32)
            d_probs = jnp.dot(value, d_out, preferred_element_type=F32)
            return q_unit, q_scale, query_t, d_out, scores, d_probs

        ahead = begin(0)
        for head in range(group):
            q_unit, q_scale, query_t, d_out, scores, d_probs = ahead
            if head + 1 < group:
                ahead = begin(head + 1)
            probs, d_scores = softmax_and_grad(scores, d_probs, causal, empty)
            mix_ref[mixed_rows(head), :] = jnp.dot(value_t, probs, preferred_element_type=F32).astype(BF16)
            d_query = jnp.dot(key_small_t, d_scores, preferred_element_type=F32)
            d_key += lax.dot_general(query_t, d_scores, NT, preferred_element_type=F32)
            d_value += lax.dot_general(d_out, probs, NT, preferred_element_type=F32)
            pull += put(head, rotate_back(head_norm_back(d_query, q_unit, q_scale), cosine, sine))
        pull += put(group, rotate_back(head_norm_back(d_key * dim**-0.5, k_unit, k_scale), cosine, sine))
        return pull + put(group + 1, d_value)

    pull = lax.fori_loop(0, kv_heads, one_kv_head, jnp.zeros((dim, tokens), F32))
    pull = jnp.sum(pull, axis=0, keepdims=True)
    pull_ref[...] = jnp.broadcast_to(pull, (LANES, tokens)).T


def attention(raw, d_mixed_t, cosine, sine, kv_heads, group, dim):
    steps, features, tokens = raw.shape
    width = kv_heads * group * dim
    pairs = steps * kv_heads * group * tokens * tokens
    return pl.pallas_call(
        functools.partial(attention_kernel, kv_heads, group, dim),
        grid=(steps,),
        in_specs=[
            pl.BlockSpec((1, features, tokens), lambda w: (w, 0, 0)),
            pl.BlockSpec((width, tokens), lambda w: (0, w)),
            pl.BlockSpec((dim // 2, tokens), lambda w: (0, w % WINDOWS)),
            pl.BlockSpec((dim // 2, tokens), lambda w: (0, w % WINDOWS)),
        ],
        out_specs=[
            pl.BlockSpec((width, tokens), lambda w: (0, w)),
            pl.BlockSpec((features, tokens), lambda w: (0, w)),
            pl.BlockSpec((tokens, LANES), lambda w: (w, 0)),
        ],
        out_shape=[
            jax.ShapeDtypeStruct((width, steps * tokens), BF16),
            jax.ShapeDtypeStruct((features, steps * tokens), BF16),
            jax.ShapeDtypeStruct((steps * tokens, LANES), F32),
        ],
        cost_estimate=pl.CostEstimate(flops=12 * pairs * dim, bytes_accessed=8 * raw.size, transcendentals=pairs),
        name='attention',
    )(raw, d_mixed_t, cosine, sine)


def input_grad_kernel(depth, place_ref, draw_ref, weight_ref, x_ref, dh_ref, gain_ref, scale_ref, pull_ref, sorted_ref, dgain_ref, d_normed, wide, sems):
    step, steps = pl.program_id(0), pl.num_programs(0)
    rows, width = x_ref.shape
    slabs = width // LANES
    slot = lax.rem(step, 2)

    def drain(which):
        pltpu.make_async_copy(wide.at[which], sorted_ref.at[pl.ds(0, rows * slabs)], sems.at[which]).wait()

    d_normed[...] = jnp.dot(draw_ref[...].T, weight_ref[...], preferred_element_type=F32)
    scale = scale_ref[...]
    pull = pull_ref[...] * scale * (1.0 / depth)

    @pl.when(step == 0)
    def _():
        dgain_ref[...] = jnp.zeros_like(dgain_ref)

    @pl.when(step >= 2)
    def _():
        drain(slot)

    for j in range(slabs):
        cols = slice(j * LANES, (j + 1) * LANES)
        x_part = x_ref[:, cols].astype(F32)
        d_part = d_normed[:, cols]
        dx_part = dh_ref[:, cols].astype(F32) + scale * (d_part * gain_ref[:, cols] - x_part * pull)
        wide[slot, pl.ds(j, rows, stride=slabs), :] = dx_part
        terms = d_part * (x_part * scale)
        dgain_ref[:, cols] += jnp.sum(terms.reshape(rows // 8, 8, LANES), axis=0)

    def one(t, carry):
        source = wide.at[slot, pl.ds(pl.multiple_of(t * slabs, slabs), slabs)]
        start = pl.multiple_of(place_ref[step * rows + t] * slabs, slabs)
        pltpu.make_async_copy(source, sorted_ref.at[pl.ds(start, slabs)], sems.at[slot]).start()
        return carry

    lax.fori_loop(0, rows, one, 0, unroll=8)

    @pl.when(step == steps - 1)
    def _():
        drain(1 - slot)
        drain(slot)


def input_grad(place, draw_t, weight_t, x, dh, gain, scale, pull, half, spare):
    tokens, depth = x.shape
    width = depth // HALVES
    slabs = width // LANES
    features = draw_t.shape[0]
    steps = tokens // ROWS
    return pl.pallas_call(
        functools.partial(input_grad_kernel, depth),
        grid_spec=pltpu.PrefetchScalarGridSpec(
            num_scalar_prefetch=1,
            grid=(steps,),
            in_specs=[
                pl.BlockSpec((features, ROWS), lambda i, place: (0, i)),
                pl.BlockSpec((features, width), lambda i, place: (0, half)),
                pl.BlockSpec((ROWS, width), lambda i, place: (i, half)),
                pl.BlockSpec((ROWS, width), lambda i, place: (i, half)),
                pl.BlockSpec((1, width), lambda i, place: (0, half)),
                pl.BlockSpec((ROWS, LANES), lambda i, place: (i, 0)),
                pl.BlockSpec((ROWS, LANES), lambda i, place: (i, 0)),
            ],
            out_specs=[
                pl.BlockSpec(memory_space=pl.ANY),
                pl.BlockSpec((8, width), lambda i, place: (0, 0)),
            ],
            scratch_shapes=[
                pltpu.VMEM((ROWS, width), F32),
                pltpu.VMEM((2, ROWS * slabs, LANES), F32),
                pltpu.SemaphoreType.DMA((2,)),
            ],
        ),
        out_shape=[
            jax.ShapeDtypeStruct(((tokens + spare) * slabs, LANES), F32),
            jax.ShapeDtypeStruct((8, width), F32),
        ],
        cost_estimate=pl.CostEstimate(flops=2 * tokens * width * features, bytes_accessed=tokens * (8 * width + 2 * features), transcendentals=0),
        name='input_grad',
    )(place, draw_t, weight_t, x, dh, gain, scale, pull)


def table_grad_kernel(bounds_ref, same_ref, target_ref, sorted_ref, zero_ref, out_ref, fetched, summed, in_sems, out_sems):
    del zero_ref
    slabs = out_ref.shape[1]
    first, last = bounds_ref[0], bounds_ref[1]
    steps = lax.div(last - first + (RUN - 1), RUN)

    def fetch(step, slot):
        start = pl.multiple_of((first + step * RUN) * slabs, slabs)
        return pltpu.make_async_copy(sorted_ref.at[pl.ds(start, RUN * slabs)], fetched.at[slot], in_sems.at[slot])

    def drain(count, slot):
        for bit in range(RUN.bit_length()):

            @pl.when(lax.rem(lax.div(count, 1 << bit), 2) == 1)
            def _():
                pltpu.make_async_copy(summed.at[slot, pl.ds(0, 1 << bit)], out_ref.at[pl.ds(0, 1 << bit)], out_sems.at[slot]).wait()

    @pl.when(steps > 0)
    def _():
        fetch(0, 0).start()

    def step_body(step, carry):
        total, older, newer = carry
        slot = lax.rem(step, 2)

        @pl.when(step + 1 < steps)
        def _():
            fetch(step + 1, 1 - slot).start()

        fetch(step, slot).wait()
        drain(older, slot)
        base = first + step * RUN

        def add(t, total):
            row = fetched[slot, pl.ds(pl.multiple_of(t * slabs, slabs), slabs), :]
            total = row + jnp.where(same_ref[base + t] == 1, total, 0.0)
            summed[slot, t] = total.astype(BF16)
            return total

        total = lax.fori_loop(0, RUN, add, total, unroll=8)

        def send(t, count):
            target = target_ref[base + t]
            wanted = jnp.logical_and(target >= 0, base + t < last)

            @pl.when(wanted)
            def _():
                pltpu.make_async_copy(summed.at[slot, t], out_ref.at[target], out_sems.at[slot]).start()

            return count + wanted.astype(jnp.int32)

        count = lax.fori_loop(0, RUN, send, jnp.int32(0), unroll=8)
        return total, newer, count

    zero = jnp.int32(0)
    _, older, newer = lax.fori_loop(0, steps, step_body, (jnp.zeros((slabs, LANES), F32), zero, zero))
    drain(older, lax.rem(steps, 2))
    drain(newer, lax.rem(steps + 1, 2))


def table_grad(bounds, same, target, sorted_rows, zero_part):
    rows, slabs, _ = zero_part.shape
    return pl.pallas_call(
        table_grad_kernel,
        grid_spec=pltpu.PrefetchScalarGridSpec(
            num_scalar_prefetch=3,
            grid=(),
            in_specs=[pl.BlockSpec(memory_space=pl.ANY), pl.BlockSpec(memory_space=pl.ANY)],
            out_specs=pl.BlockSpec(memory_space=pl.ANY),
            scratch_shapes=[
                pltpu.VMEM((2, RUN * slabs, LANES), F32),
                pltpu.VMEM((2, RUN, slabs, LANES), BF16),
                pltpu.SemaphoreType.DMA((2,)),
                pltpu.SemaphoreType.DMA((2,)),
            ],
        ),
        out_shape=jax.ShapeDtypeStruct((rows, slabs, LANES), BF16),
        input_output_aliases={4: 0},
        cost_estimate=pl.CostEstimate(flops=sorted_rows.size // PARTS, bytes_accessed=6 * sorted_rows.size // PARTS, transcendentals=0),
        name='table_grad',
    )(bounds, same, target, sorted_rows, zero_part)


def pair_sum_kernel(part_ref, out_ref, came, mine, send_sems, recv_sems, in_sems, out_sems):
    chips, rows = came.shape[:2]
    me = lax.axis_index('fsdp')
    core = lax.rem(me, 2)
    partner = me + 1 - 2 * core
    barrier = pltpu.get_barrier_semaphore()
    pl.semaphore_signal(barrier, inc=1, device_id=(partner,), device_id_type=pl.DeviceIdType.MESH)
    pl.semaphore_wait(barrier, 1)
    sends, loads, stores = [], [], []
    for q in range(chips):
        sends.append(
            pltpu.make_async_remote_copy(
                src_ref=part_ref.at[pl.ds((2 * q + 1 - core) * rows, rows)],
                dst_ref=came.at[q],
                send_sem=send_sems.at[q],
                recv_sem=recv_sems.at[q],
                device_id=(partner,),
                device_id_type=pl.DeviceIdType.MESH,
            )
        )
        loads.append(pltpu.make_async_copy(part_ref.at[pl.ds((2 * q + core) * rows, rows)], mine.at[q], in_sems.at[q]))
        stores.append(pltpu.make_async_copy(mine.at[q], out_ref.at[pl.ds(q * rows, rows)], out_sems.at[q]))
        sends[q].start()
        loads[q].start()
    for q in range(chips):
        loads[q].wait()
        sends[q].wait_recv()

        def add(i, carry):
            at = pl.ds(i * 8, 8)
            mine[q, at] = (mine[q, at].astype(F32) + came[q, at].astype(F32)).astype(BF16)
            return carry

        lax.fori_loop(0, rows // 8, add, 0)
        stores[q].start()
    for q in range(chips):
        stores[q].wait()
        sends[q].wait_send()


def pair_sum(part, index, devices):
    total, slabs, _ = part.shape
    chips, rows = devices // 2, total // devices
    return pl.pallas_call(
        pair_sum_kernel,
        out_shape=jax.ShapeDtypeStruct((chips * rows, slabs, LANES), BF16),
        in_specs=[pl.BlockSpec(memory_space=pl.ANY)],
        out_specs=pl.BlockSpec(memory_space=pl.ANY),
        scratch_shapes=[
            pltpu.VMEM((chips, rows, slabs, LANES), BF16),
            pltpu.VMEM((chips, rows, slabs, LANES), BF16),
            pltpu.SemaphoreType.DMA((chips,)),
            pltpu.SemaphoreType.DMA((chips,)),
            pltpu.SemaphoreType.DMA((chips,)),
            pltpu.SemaphoreType.DMA((chips,)),
        ],
        compiler_params=pltpu.CompilerParams(collective_id=index),
        cost_estimate=pl.CostEstimate(flops=part.size, bytes_accessed=4 * part.size, transcendentals=0),
        name='pair_sum',
    )(part)


def zero_kernel(*refs):
    *out_refs, block, sem = refs
    block[...] = jnp.zeros_like(block)
    rows = block.shape[0]
    copies = [pltpu.make_async_copy(block, ref.at[pl.ds(start, rows)], sem) for ref in out_refs for start in range(0, ref.shape[0], rows)]
    for copy in copies:
        copy.start()
    for copy in copies:
        copy.wait()


def zero_tables(count, rows, slabs, block=400):
    return pl.pallas_call(
        zero_kernel,
        out_shape=[jax.ShapeDtypeStruct((rows, slabs, LANES), BF16)] * count,
        out_specs=[pl.BlockSpec(memory_space=pl.ANY)] * count,
        scratch_shapes=[pltpu.VMEM((block, slabs, LANES), BF16), pltpu.SemaphoreType.DMA],
        cost_estimate=pl.CostEstimate(flops=count * rows * slabs * LANES, bytes_accessed=2 * count * rows * slabs * LANES, transcendentals=0),
        name='zero_tables',
    )()


def solution(mesh):
    devices = mesh.shape['fsdp']

    def device_step(token_ids, embed_table, norm_gain, w_query, w_key, w_value, w_out, grad_out):
        batch, seq_len = token_ids.shape
        table_rows, width = embed_table.shape
        heads, dim = w_query.shape[1], w_query.shape[2]
        kv_heads = w_key.shape[1]
        group = heads // kv_heads
        tokens = batch * seq_len
        slabs = width // LANES
        ids = token_ids.reshape(tokens)
        dh = grad_out.reshape(tokens, width)

        def grouped(w, count):
            return w.transpose(1, 2, 0).reshape(kv_heads, count * dim, -1)

        weight_part = jnp.concatenate([grouped(w_query, group), grouped(w_key, 1), grouped(w_value, 1)], axis=1)
        weight_part = weight_part.reshape(-1, weight_part.shape[-1])
        wout_full = lax.all_gather(w_out, 'fsdp', axis=0, tiled=True)
        weight_t = lax.all_gather(weight_part, 'fsdp', axis=1, tiled=True)
        gain = lax.all_gather(norm_gain, 'fsdp', axis=0, tiled=True).astype(F32).reshape(1, width)
        table = lax.all_gather(split_rows(embed_table), 'fsdp', axis=0, tiled=True)

        piece = table_rows // PARTS
        part_rows = piece * devices
        local = ids % table_rows
        key = (local // piece) * part_rows + (ids // table_rows) * piece + local % piece
        count = jnp.arange(tokens, dtype=jnp.int32)
        sorted_key, order = lax.sort((key, count), num_keys=1)
        _, place = lax.sort((order, count), num_keys=1)
        outside = jnp.full((1,), -1, jnp.int32)
        same = (sorted_key == jnp.concatenate([outside, sorted_key[:-1]])).astype(jnp.int32)
        ends = sorted_key != jnp.concatenate([sorted_key[1:], outside])
        target = jnp.where(ends, sorted_key % part_rows, -1)
        spare = jnp.zeros((RUN,), jnp.int32)
        same = jnp.concatenate([same, spare])
        target = jnp.concatenate([target, spare - 1])
        bounds = jnp.sum(key[None, :] < part_rows * jnp.arange(PARTS + 1, dtype=jnp.int32)[:, None], axis=1, dtype=jnp.int32)

        half = dim // 2
        frequency = ROPE_THETA ** (-2.0 * jnp.arange(half, dtype=F32) / dim)
        angles = frequency[:, None] * jnp.arange(seq_len, dtype=F32)[None, :]
        cosine, sine = jnp.cos(angles), jnp.sin(angles)

        d_mixed_t = lax.dot_general(wout_full, dh, NT, preferred_element_type=F32).astype(BF16)
        half_slabs = slabs // HALVES
        zero_parts = zero_tables(PARTS * HALVES, part_rows, half_slabs)
        d_mixed_t, *zero_parts = lax.optimization_barrier((d_mixed_t, *zero_parts))

        x, normed, scale, raw = embed_project(ids, table, gain, weight_t)
        mixed_t, draw_t, pull = attention(raw, d_mixed_t, cosine, sine, kv_heads, group, dim)
        same_core = [list(range(core, devices, 2)) for core in range(2)]
        dgains, shares, sums = [], [], []
        for h in range(HALVES):
            if sums:
                pull, *_ = lax.optimization_barrier((pull, *sums))
            sorted_rows, dgain = input_grad(place, draw_t, weight_t, x, dh, gain, scale, pull, h, RUN)
            dgains.append(jnp.sum(dgain, axis=0))
            for k in range(PARTS):
                index = h * PARTS + k
                part = table_grad(bounds[k : k + 2], same, target, sorted_rows, zero_parts[index])
                sums.append(pair_sum(part, index, devices))
                shares.append(lax.psum_scatter(sums[-1], 'fsdp', scatter_dimension=0, tiled=True, axis_index_groups=same_core))
        grad_table = None
        for h in range(HALVES):
            for k in range(PARTS):
                grad_table = join_rows(shares[h * PARTS + k], grad_table, h, k, 1.0 / devices)

        mixed_t, draw_t, *_ = lax.optimization_barrier((mixed_t, draw_t, *sums))
        grad_weight = jnp.dot(draw_t, normed, preferred_element_type=F32).astype(BF16)
        grad_weight = lax.psum_scatter(grad_weight, 'fsdp', scatter_dimension=1, tiled=True)
        grad_weight = grad_weight.astype(F32) / devices
        grad_wout = jnp.dot(mixed_t, dh, preferred_element_type=F32).astype(BF16)
        grad_wout = lax.psum_scatter(grad_wout, 'fsdp', scatter_dimension=0, tiled=True)
        grad_wout = grad_wout.astype(F32) / devices
        hidden = x.astype(F32) + lax.dot_general(mixed_t, wout_full, (((0,), (0,)), ((), ())), preferred_element_type=F32)
        hidden = hidden.astype(BF16).reshape(batch, seq_len, width)
        grad_gain = lax.psum_scatter(jnp.concatenate(dgains), 'fsdp', scatter_dimension=0, tiled=True) / devices

        grad_weight = grad_weight.reshape(kv_heads, (group + 2) * dim, -1)

        def ungrouped(part, count):
            return part.reshape(kv_heads * count, dim, -1).transpose(2, 0, 1)

        grad_query = ungrouped(grad_weight[:, : group * dim], group)
        grad_key = ungrouped(grad_weight[:, group * dim : (group + 1) * dim], 1)
        grad_value = ungrouped(grad_weight[:, (group + 1) * dim :], 1)
        return hidden, grad_table, grad_gain, grad_query, grad_key, grad_value, grad_wout

    tokens = P('fsdp', None, None)
    matrix = P('fsdp', None)
    vector = P('fsdp')
    return jax.shard_map(device_step, mesh=mesh, in_specs=(matrix, matrix, vector, tokens, tokens, tokens, matrix, tokens), out_specs=(tokens, matrix, vector, tokens, tokens, tokens, matrix), check_vma=False)
```
